16 devices in a mesh: dp: 2 (over z), sp: 8 (over y, x, core).
Axes of the slice: x: 2, y: 2, z: 2, core: 2. Of those that a mesh axis runs over, the one named last changes fastest.
Arguments:
- x: bfloat16 [64, 512, 128], P('dp', 'sp'), parts along dimension 0
- w_cur: bfloat16 [16, 8, 128, 256], replicated
- w_past: bfloat16 [16, 8, 128, 256], replicated
- w_res: bfloat16 [16, 8, 128, 128], replicated
- w_skip: bfloat16 [16, 8, 128, 128], replicated
Outputs:
- output 1: float32 [64, 8, 64, 128], P('dp', 'sp'), parts along dimension 0
- output 2: float32 [64, 8, 64, 128], P('dp', 'sp'), parts along dimension 0
There are 2 independent parts. The reference program is written for one: setup_inputs(seed, part) draws one part's arguments, and reference() takes and returns one part's arrays. A program takes and returns all parts, laid end to end along the dimension named above; an argument that names none is the same for every part.
All inputs are finite; a program needn't handle non-finite values.
Results may differ from the reference program's by a relative error of at most 0.00860394.
Values are sent between devices in bfloat16 or wider.
A program may use at most 1 GiB of HBM per device.

```python
import jax
import jax.numpy as jnp
from jax import lax

BATCH_PART = 32
SEQ_DEV = 64
GROUP_SIZE = 8
STACKS = 16
CHANNELS = 128
SKIP_CH = 128
CYCLE_LEN = 8

SEQ_LEN = SEQ_DEV * GROUP_SIZE
LAYERS = STACKS * CYCLE_LEN


def setup_inputs(seed: int = 0, part: int = 0) -> dict:
    base_key = jax.random.key(seed)
    key_x = jax.random.fold_in(jax.random.fold_in(base_key, 1), part)
    key_w = jax.random.split(jax.random.fold_in(base_key, 2), 4)
    tap_scale = (2 * CHANNELS) ** -0.5
    out_scale = 2.0 * (CHANNELS * LAYERS) ** -0.5
    tap_shape = (STACKS, CYCLE_LEN, CHANNELS, 2 * CHANNELS)
    x = jax.random.normal(key_x, (BATCH_PART, SEQ_LEN, CHANNELS), jnp.float32)
    w_cur = jax.random.normal(key_w[0], tap_shape, jnp.float32) * tap_scale
    w_past = jax.random.normal(key_w[1], tap_shape, jnp.float32) * tap_scale
    w_res = jax.random.normal(key_w[2], (STACKS, CYCLE_LEN, CHANNELS, CHANNELS), jnp.float32) * out_scale
    w_skip = jax.random.normal(key_w[3], (STACKS, CYCLE_LEN, CHANNELS, SKIP_CH), jnp.float32) * out_scale
    return {"x": x.astype(jnp.bfloat16), "w_cur": w_cur.astype(jnp.bfloat16), "w_past": w_past.astype(jnp.bfloat16), "w_res": w_res.astype(jnp.bfloat16), "w_skip": w_skip.astype(jnp.bfloat16)}


def gated_layer(h_res, skip_acc, cur_w, past_w, res_w, skip_w, dilation):
    row_count = BATCH_PART * SEQ_LEN
    u_cur = h_res.astype(jnp.bfloat16)
    u_past = jnp.concatenate([jnp.zeros((BATCH_PART, dilation, CHANNELS), jnp.bfloat16), u_cur[:, :SEQ_LEN - dilation]], axis=1)
    pre_act = jnp.dot(u_cur.reshape(row_count, CHANNELS), cur_w, preferred_element_type=jnp.float32) + jnp.dot(u_past.reshape(row_count, CHANNELS), past_w, preferred_element_type=jnp.float32)
    gated = (jnp.tanh(pre_act[:, :CHANNELS]) * jax.nn.sigmoid(pre_act[:, CHANNELS:])).astype(jnp.bfloat16)
    h_new = h_res + jnp.dot(gated, res_w, preferred_element_type=jnp.float32).reshape(BATCH_PART, SEQ_LEN, CHANNELS)
    skip_new = skip_acc + jnp.dot(gated, skip_w, preferred_element_type=jnp.float32).reshape(BATCH_PART, SEQ_LEN, SKIP_CH)
    return h_new, skip_new


def reference(x, w_cur, w_past, w_res, w_skip):
    def stack_body(carry, weights):
        h_res, skip_acc = carry
        stack_cur, stack_past, stack_res, stack_skip = weights
        for layer_pos in range(CYCLE_LEN):
            h_res, skip_acc = gated_layer(h_res, skip_acc, stack_cur[layer_pos], stack_past[layer_pos], stack_res[layer_pos], stack_skip[layer_pos], 2 ** layer_pos)
        return (h_res, skip_acc), None

    h_start = x.astype(jnp.float32)
    skip_start = jnp.zeros((BATCH_PART, SEQ_LEN, SKIP_CH), jnp.float32)
    (h_fin, skip_fin), unused = lax.scan(stack_body, (h_start, skip_start), (w_cur, w_past, w_res, w_skip))
    h_out = h_fin.reshape(BATCH_PART, SEQ_DEV, GROUP_SIZE, CHANNELS).transpose(0, 2, 1, 3)
    skip_out = skip_fin.reshape(BATCH_PART, SEQ_DEV, GROUP_SIZE, SKIP_CH).transpose(0, 2, 1, 3)
    return (h_out, skip_out)
```

```python
import functools

import jax
import jax.numpy as jnp
from jax import lax
from jax.experimental import pallas as pl
from jax.experimental.pallas import tpu as pltpu
from jax.sharding import PartitionSpec as P

MESH = pl.DeviceIdType.MESH
ROWS = 128
ZPAD = 128
HPAD = 8
F32 = jnp.float32
BF16 = jnp.bfloat16


def kernel(group_n, seqs, seq_len, stacks, cycle_len, x_ref, wc_hbm, wp_hbm, wr_hbm, ws_hbm, h_out, s_out,
           xin, h_buf, u_buf, skip, wc, wp, wr, ws, h_st, s_st,
           in_send, in_recv, out_send, out_recv, w_sem, own_sem):
    me = lax.axis_index("sp")
    seq_dev = seq_len // group_n
    weights = ((wc_hbm, wc), (wp_hbm, wp), (wr_hbm, wr), (ws_hbm, ws))

    def weight_copy(stack, which):
        src, dst = weights[which]
        return pltpu.make_async_copy(src.at[stack], dst.at[stack], w_sem.at[which, stack])

    barrier = pltpu.get_barrier_semaphore()
    for step in range(1, group_n):
        pl.semaphore_signal(barrier, inc=1, device_id={"sp": lax.rem(me + step, group_n)}, device_id_type=MESH)
    own_in = pltpu.make_async_copy(x_ref.at[pl.ds(me * seqs, seqs)], xin.at[:, pl.ds(me * seq_dev, seq_dev)], own_sem.at[0])
    own_in.start()
    for which in range(4):
        weight_copy(0, which).start()
    pl.semaphore_wait(barrier, group_n - 1)

    in_copies = []
    for step in range(1, group_n):
        peer = lax.rem(me + step, group_n)
        copy = pltpu.make_async_remote_copy(
            src_ref=x_ref.at[pl.ds(peer * seqs, seqs)], dst_ref=xin.at[:, pl.ds(me * seq_dev, seq_dev)],
            send_sem=in_send.at[step - 1], recv_sem=in_recv.at[step - 1], device_id={"sp": peer}, device_id_type=MESH)
        copy.start()
        in_copies.append(copy)
    for stack in range(1, stacks):
        for which in range(4):
            weight_copy(stack, which).start()

    zeros_z = jnp.zeros((ZPAD, 128), BF16)
    zeros_h = jnp.zeros((HPAD, 128), F32)
    for b in range(seqs):
        for side in range(2):
            u_buf[side, b, 0:ZPAD, :] = zeros_z
            h_buf[side, b, 0:HPAD, :] = zeros_h
    own_in.wait()
    for copy in in_copies:
        copy.wait()

    chunks = [(b, q) for q in range(seq_len // ROWS) for b in range(seqs)]
    for b, q in chunks:
        piece = xin[b, q * ROWS:(q + 1) * ROWS, :]
        u_buf[0, b, ZPAD + q * ROWS:ZPAD + (q + 1) * ROWS, :] = piece
        h_buf[0, b, HPAD + q * ROWS:HPAD + (q + 1) * ROWS, :] = piece.astype(F32)
        skip[b, q * ROWS:(q + 1) * ROWS, :] = jnp.zeros((ROWS, 128), F32)

    def past(side, b, q, dilation):
        if dilation < 16:
            start = HPAD + q * ROWS - dilation
            return h_buf[side, b, start:start + ROWS, :].astype(BF16)
        start = ZPAD + q * ROWS - dilation
        return u_buf[side, b, start:start + ROWS, :]

    n_acc = 1024 // ROWS

    def body(*accs):
        acc_z, acc_r = accs[:n_acc], accs[n_acc:]

        def stack_body(stack, carry):
            for which in range(4):
                weight_copy(stack, which).wait()
            zs, rs = {}, {}

            def do_z(layer, c):
                b, q = chunks[c]
                side = layer % 2
                u = u_buf[side, b, ZPAD + q * ROWS:ZPAD + (q + 1) * ROWS, :]
                lhs = jnp.concatenate([u, past(side, b, q, 2 ** layer)], axis=1)
                zs[layer, c] = jnp.dot(lhs, jnp.concatenate([wc[stack, layer], wp[stack, layer]], axis=0), preferred_element_type=F32)

            def do_gate(layer, c):
                z = zs.pop((layer, c))
                a = (jnp.tanh(z[:, :128]) * jax.nn.sigmoid(z[:, 128:])).astype(BF16)
                top = jnp.concatenate([wr[stack, layer], ws[stack, layer]], axis=1)
                rs[layer, c] = jnp.dot(a, top, preferred_element_type=F32)

            def do_update(layer, c):
                b, q = chunks[c]
                side = layer % 2
                r = rs.pop((layer, c))
                h_rows = slice(HPAD + q * ROWS, HPAD + (q + 1) * ROWS)
                h_new = h_buf[side, b, h_rows, :] + r[:, :128]
                h_buf[1 - side, b, h_rows, :] = h_new
                u_buf[1 - side, b, ZPAD + q * ROWS:ZPAD + (q + 1) * ROWS, :] = h_new.astype(BF16)
                s_rows = slice(q * ROWS, (q + 1) * ROWS)
                skip[b, s_rows, :] = skip[b, s_rows, :] + r[:, 128:]

            tasks = [(layer, c) for layer in range(cycle_len) for c in range(len(chunks))]
            lag1, lag2 = 4, 8
            for k in range(len(tasks) + lag2):
                if k < len(tasks):
                    do_z(*tasks[k])
                if 0 <= k - lag1 < len(tasks):
                    do_gate(*tasks[k - lag1])
                if 0 <= k - lag2 < len(tasks):
                    do_update(*tasks[k - lag2])
            return carry

        lax.fori_loop(0, stacks, stack_body, 0)

    body()

    for j in range(group_n):
        for b in range(seqs):
            h_st[j, b] = h_buf[0, b, pl.ds(HPAD + j, seq_dev, stride=group_n), :]
            s_st[j, b] = skip[b, pl.ds(j, seq_dev, stride=group_n), :]
    copies = []
    for step in range(1, group_n):
        peer = lax.rem(me + step, group_n)
        for which, (src, dst) in enumerate(((h_st, h_out), (s_st, s_out))):
            copy = pltpu.make_async_remote_copy(
                src_ref=src.at[peer], dst_ref=dst.at[pl.ds(me * seqs, seqs)],
                send_sem=out_send.at[which, step - 1], recv_sem=out_recv.at[which, step - 1], device_id={"sp": peer}, device_id_type=MESH)
            copy.start()
            copies.append(copy)
    for which, (src, dst) in enumerate(((h_st, h_out), (s_st, s_out))):
        copy = pltpu.make_async_copy(src.at[me], dst.at[pl.ds(me * seqs, seqs)], own_sem.at[1 + which])
        copy.start()
        copies.append(copy)
    for copy in copies:
        copy.wait()


def solution(mesh):
    group_n = mesh.shape["sp"]

    def local(x_loc, w_cur, w_past, w_res, w_skip):
        batch, seq_dev, channels = x_loc.shape
        stacks, cycle_len = w_cur.shape[:2]
        seqs, seq_len = batch // group_n, seq_dev * group_n
        any_spec = pl.BlockSpec(memory_space=pl.ANY)
        out = jax.ShapeDtypeStruct((batch, seq_dev, channels), F32)
        h_out, s_out = pl.pallas_call(
            functools.partial(kernel, group_n, seqs, seq_len, stacks, cycle_len),
            out_shape=(out, out),
            in_specs=[any_spec] * 5,
            out_specs=(any_spec, any_spec),
            scratch_shapes=[
                pltpu.VMEM((seqs, seq_len, channels), BF16),
                pltpu.VMEM((2, seqs, HPAD + seq_len, channels), F32),
                pltpu.VMEM((2, seqs, ZPAD + seq_len, channels), BF16),
                pltpu.VMEM((seqs, seq_len, channels), F32),
                pltpu.VMEM(w_cur.shape, BF16),
                pltpu.VMEM(w_past.shape, BF16),
                pltpu.VMEM(w_res.shape, BF16),
                pltpu.VMEM(w_skip.shape, BF16),
                pltpu.VMEM((group_n, seqs, seq_dev, channels), F32),
                pltpu.VMEM((group_n, seqs, seq_dev, channels), F32),
                pltpu.SemaphoreType.DMA((group_n - 1,)),
                pltpu.SemaphoreType.DMA((group_n - 1,)),
                pltpu.SemaphoreType.DMA((2, group_n - 1)),
                pltpu.SemaphoreType.DMA((2, group_n - 1)),
                pltpu.SemaphoreType.DMA((4, stacks)),
                pltpu.SemaphoreType.DMA((3,)),
            ],
            compiler_params=pltpu.CompilerParams(collective_id=0, has_side_effects=True, vmem_limit_bytes=60 * 1024 * 1024),
        )(x_loc, w_cur, w_past, w_res, w_skip)
        return h_out.reshape(batch, 1, seq_dev, channels), s_out.reshape(batch, 1, seq_dev, channels)

    return jax.shard_map(local, mesh=mesh, in_specs=(P("dp", "sp", None), P(), P(), P(), P()), out_specs=(P("dp", "sp", None, None), P("dp", "sp", None, None)), check_vma=False)
```

```python
import functools

import jax
import jax.numpy as jnp
from jax import lax
from jax.experimental import pallas as pl
from jax.experimental.pallas import tpu as pltpu
from jax.sharding import PartitionSpec as P

MESH = pl.DeviceIdType.MESH
ROWS = 128
ZPAD = 128
HPAD = 8
GROUPS = 2
LEAD = 5
VMEM_MIB = 40
SOLO = (128, 3, 6)
BOTH = (256, 2, 4)
F32 = jnp.float32
BF16 = jnp.bfloat16


def kernel(group_n, seqs, seq_len, stacks, cycle_len, x_ref, wc_hbm, wp_hbm, wr_hbm, ws_hbm, h_out, s_out,
           xin, h_buf, u_buf, a_buf, skip, wc, wp, wr, ws, h_st, s_st,
           in_send, in_recv, out_send, out_recv, w_sem, own_sem):
    me = lax.axis_index("sp")
    seq_dev = seq_len // group_n
    part = seqs // GROUPS
    peers = {}
    for flip in range(1, group_n):
        peer, unit = 0, 1
        while unit < group_n:
            bit = lax.rem(me // unit, 2)
            peer = peer + unit * (1 - bit if flip // unit % 2 else bit)
            unit *= 2
        peers[flip] = peer
    order = sorted(peers, reverse=True)
    weights = ((wc_hbm, wc), (wp_hbm, wp), (wr_hbm, wr), (ws_hbm, ws))

    def weight_copy(stack, which):
        src, dst = weights[which]
        return pltpu.make_async_copy(src.at[stack], dst.at[stack], w_sem.at[which, stack])

    barrier = pltpu.get_barrier_semaphore()
    for flip in order:
        pl.semaphore_signal(barrier, inc=1, device_id={"sp": peers[flip]}, device_id_type=MESH)
    own_in = pltpu.make_async_copy(x_ref.at[pl.ds(me * seqs, seqs)], xin.at[:, pl.ds(me * seq_dev, seq_dev)], own_sem.at[0])
    own_in.start()
    for which in range(4):
        weight_copy(0, which).start()
    zeros_z = jnp.zeros((ZPAD, 128), BF16)
    zeros_h = jnp.zeros((HPAD, 128), F32)
    for b in range(seqs):
        for side in range(2):
            u_buf[side, b, 0:ZPAD, :] = zeros_z
            h_buf[side, b, 0:HPAD, :] = zeros_h
        skip[b] = jnp.zeros((seq_len, 128), F32)
    pl.semaphore_wait(barrier, group_n - 1)

    in_copies = [[] for _ in range(GROUPS)]
    for g in range(GROUPS):
        for flip in order:
            peer = peers[flip]
            copy = pltpu.make_async_remote_copy(
                src_ref=x_ref.at[pl.ds(peer * seqs + g * part, part)],
                dst_ref=xin.at[pl.ds(g * part, part), pl.ds(me * seq_dev, seq_dev)],
                send_sem=in_send.at[g, flip - 1], recv_sem=in_recv.at[g, flip - 1], device_id={"sp": peer}, device_id_type=MESH)
            copy.start()
            in_copies[g].append(copy)
    for stack in range(1, stacks):
        for which in range(4):
            weight_copy(stack, which).start()

    own_in.wait()

    def past(side, b, first, rows, dilation):
        if dilation < 16:
            start = HPAD + first - dilation
            return h_buf[side, b, start:start + rows, :].astype(BF16)
        start = ZPAD + first - dilation
        return u_buf[side, b, start:start + rows, :]

    def load_input(g):
        for copy in in_copies[g]:
            copy.wait()
        for b in range(g * part, (g + 1) * part):
            for q in range(seq_len // ROWS):
                piece = xin[b, q * ROWS:(q + 1) * ROWS, :]
                u_buf[0, b, ZPAD + q * ROWS:ZPAD + (q + 1) * ROWS, :] = piece
                h_buf[0, b, HPAD + q * ROWS:HPAD + (q + 1) * ROWS, :] = piece.astype(F32)

    def run(streams, rows, lag1, lag2, paired=True):
        tasks = []
        for k in range(max(len(layers) for _, layers in streams)):
            for g, layers in streams:
                per = max(len(other) for _, other in streams) // len(layers)
                cells = [(b, q) for q in range(seq_len // rows) for b in range(g * part, (g + 1) * part)]
                share = len(cells) // per
                stack, layer = layers[k // per]
                tasks += [(stack, layer, b, q) for b, q in cells[k % per * share:(k % per + 1) * share]]
        zs, rs, gs = {}, {}, []

        def do_z(stack, layer, b, q):
            side = layer % 2
            u = u_buf[side, b, ZPAD + q * rows:ZPAD + (q + 1) * rows, :]
            lhs = jnp.concatenate([u, past(side, b, q * rows, rows, 2 ** layer)], axis=1)
            zs[b, q] = jnp.dot(lhs, jnp.concatenate([wc[stack, layer], wp[stack, layer]], axis=0), preferred_element_type=F32)

        def do_gate(stack, layer, b, q):
            z = zs.pop((b, q))
            a = (jnp.tanh(z[:, :128]) * jax.nn.sigmoid(z[:, 128:])).astype(BF16)
            span = slice(q * rows, (q + 1) * rows)
            w_res = wr[stack, layer]
            zero = jnp.zeros_like(w_res)
            if not paired:
                r = jnp.dot(a, jnp.concatenate([w_res, ws[stack, layer]], axis=1), preferred_element_type=F32)
                rs[b, q] = r[:, :128], r[:, 128:]
            elif layer % 2 == 0:
                a_buf[b, span, :] = a
                gs.append(((b, q), a))
                if len(gs) == 2:
                    (cell0, a0), (cell1, a1) = gs
                    gs.clear()
                    diag = jnp.concatenate([jnp.concatenate([w_res, zero], axis=1), jnp.concatenate([zero, w_res], axis=1)], axis=0)
                    r = jnp.dot(jnp.concatenate([a0, a1], axis=1), diag, preferred_element_type=F32)
                    rs[cell0] = r[:, :128], None
                    rs[cell1] = r[:, 128:], None
            else:
                top = jnp.concatenate([zero, ws[stack, layer - 1]], axis=1)
                rhs = jnp.concatenate([top, jnp.concatenate([w_res, ws[stack, layer]], axis=1)], axis=0)
                r = jnp.dot(jnp.concatenate([a_buf[b, span, :], a], axis=1), rhs, preferred_element_type=F32)
                rs[b, q] = r[:, :128], r[:, 128:]

        def do_update(stack, layer, b, q):
            side = layer % 2
            dh, ds = rs.pop((b, q))
            h_rows = slice(HPAD + q * rows, HPAD + (q + 1) * rows)
            h_new = h_buf[side, b, h_rows, :] + dh
            h_buf[1 - side, b, h_rows, :] = h_new
            u_buf[1 - side, b, ZPAD + q * rows:ZPAD + (q + 1) * rows, :] = h_new.astype(BF16)
            if ds is not None:
                s_rows = slice(q * rows, (q + 1) * rows)
                skip[b, s_rows, :] = skip[b, s_rows, :] + ds

        for k in range(len(tasks) + lag2):
            if k < len(tasks):
                do_z(*tasks[k])
            if 0 <= k - lag1 < len(tasks):
                do_gate(*tasks[k - lag1])
            if 0 <= k - lag2 < len(tasks):
                do_update(*tasks[k - lag2])

    def layers_of(stack):
        return [(stack, layer) for layer in range(cycle_len)]

    def first_use(stack):
        for which in range(4):
            weight_copy(stack, which).wait()

    copies = []

    def send_output(g):
        group_rows = pl.ds(g * part, part)
        pairs = ((h_st, h_out), (s_st, s_out))

        def stage(peer):
            for b in range(g * part, (g + 1) * part):
                h_st[peer, b] = h_buf[0, b, pl.ds(HPAD + peer, seq_dev, stride=group_n), :]
                s_st[peer, b] = skip[b, pl.ds(peer, seq_dev, stride=group_n), :]

        def send(flip):
            for which, (src, dst) in enumerate(pairs):
                copy = pltpu.make_async_remote_copy(
                    src_ref=src.at[peers[flip], group_rows], dst_ref=dst.at[pl.ds(me * seqs + g * part, part)],
                    send_sem=out_send.at[g, which, flip - 1], recv_sem=out_recv.at[g, which, flip - 1],
                    device_id={"sp": peers[flip]}, device_id_type=MESH)
                copy.start()
                copies.append(copy)

        for place, flip in enumerate(order):
            stage(peers[flip])
            if place:
                send(order[place - 1])
        stage(me)
        send(order[-1])
        for which, (src, dst) in enumerate(pairs):
            copy = pltpu.make_async_copy(src.at[me, group_rows], dst.at[pl.ds(me * seqs + g * part, part)], own_sem.at[1 + 2 * g + which])
            copy.start()
            copies.append(copy)

    def only_first(stack, carry):
        first_use(stack)
        run([(0, layers_of(stack))], *SOLO)
        return carry

    def both(stack, carry):
        first_use(stack + LEAD)
        run([(0, layers_of(stack + LEAD)), (1, layers_of(stack))], *BOTH)
        return carry

    def only_second(stack, carry):
        run([(1, layers_of(stack))], *SOLO)
        return carry

    load_input(0)
    lax.fori_loop(0, LEAD, only_first, 0)
    load_input(1)
    lax.fori_loop(0, stacks - LEAD, both, 0)
    send_output(0)
    lax.fori_loop(stacks - LEAD, stacks, only_second, 0)
    send_output(1)
    for copy in copies:
        copy.wait()


def solution(mesh):
    group_n = mesh.shape["sp"]

    def local(x_loc, w_cur, w_past, w_res, w_skip):
        batch, seq_dev, channels = x_loc.shape
        stacks, cycle_len = w_cur.shape[:2]
        seqs, seq_len = batch // group_n, seq_dev * group_n
        any_spec = pl.BlockSpec(memory_space=pl.ANY)
        out = jax.ShapeDtypeStruct((batch, seq_dev, channels), F32)
        args = [pltpu.with_memory_space_constraint(v, pltpu.HBM) for v in (x_loc, w_cur, w_past, w_res, w_skip)]
        h_out, s_out = pl.pallas_call(
            functools.partial(kernel, group_n, seqs, seq_len, stacks, cycle_len),
            out_shape=(out, out),
            in_specs=[any_spec] * 5,
            out_specs=(any_spec, any_spec),
            scratch_shapes=[
                pltpu.VMEM((seqs, seq_len, channels), BF16),
                pltpu.VMEM((2, seqs, HPAD + seq_len, channels), F32),
                pltpu.VMEM((2, seqs, ZPAD + seq_len, channels), BF16),
                pltpu.VMEM((seqs, seq_len, channels), BF16),
                pltpu.VMEM((seqs, seq_len, channels), F32),
                pltpu.VMEM(w_cur.shape, BF16),
                pltpu.VMEM(w_past.shape, BF16),
                pltpu.VMEM(w_res.shape, BF16),
                pltpu.VMEM(w_skip.shape, BF16),
                pltpu.VMEM((group_n, seqs, seq_dev, channels), F32),
                pltpu.VMEM((group_n, seqs, seq_dev, channels), F32),
                pltpu.SemaphoreType.DMA((GROUPS, group_n - 1)),
                pltpu.SemaphoreType.DMA((GROUPS, group_n - 1)),
                pltpu.SemaphoreType.DMA((GROUPS, 2, group_n - 1)),
                pltpu.SemaphoreType.DMA((GROUPS, 2, group_n - 1)),
                pltpu.SemaphoreType.DMA((4, stacks)),
                pltpu.SemaphoreType.DMA((1 + 2 * GROUPS,)),
            ],
            compiler_params=pltpu.CompilerParams(collective_id=0, has_side_effects=True, vmem_limit_bytes=VMEM_MIB * 1024 * 1024),
        )(*args)
        return h_out.reshape(batch, 1, seq_dev, channels), s_out.reshape(batch, 1, seq_dev, channels)

    return jax.shard_map(local, mesh=mesh, in_specs=(P("dp", "sp", None), P(), P(), P(), P()), out_specs=(P("dp", "sp", None, None), P("dp", "sp", None, None)), check_vma=False)
```

```python
import functools

import jax
import jax.numpy as jnp
from jax import lax
from jax.experimental import pallas as pl
from jax.experimental.pallas import tpu as pltpu
from jax.sharding import PartitionSpec as P

MESH = pl.DeviceIdType.MESH
ROWS = 128
ZPAD = 128
HPAD = 8
GROUPS = 2
LEAD = 5
HEAD = 1
VMEM_MIB = 40
SOLO = (128, 3, 6)
BOTH = (256, 2, 4)
FAST = (256, 2, 5)
F32 = jnp.float32
BF16 = jnp.bfloat16


def kernel(group_n, seqs, seq_len, stacks, cycle_len, x_ref, wc_hbm, wp_hbm, wr_hbm, ws_hbm, h_out, s_out,
           xin, h_buf, u_buf, a_buf, skip, wc, wp, wr, ws, h_st, s_st,
           in_send, in_recv, out_send, out_recv, w_sem, own_sem):
    me = lax.axis_index("sp")
    seq_dev = seq_len // group_n
    part = seqs // GROUPS
    peers = {}
    for flip in range(1, group_n):
        peer, unit = 0, 1
        while unit < group_n:
            bit = lax.rem(me // unit, 2)
            peer = peer + unit * (1 - bit if flip // unit % 2 else bit)
            unit *= 2
        peers[flip] = peer
    order = sorted(peers, reverse=True)
    weights = ((wc_hbm, wc), (wp_hbm, wp), (wr_hbm, wr), (ws_hbm, ws))

    def weight_copy(stack, which):
        src, dst = weights[which]
        return pltpu.make_async_copy(src.at[stack], dst.at[stack], w_sem.at[which, stack])

    barrier = pltpu.get_barrier_semaphore()
    for flip in order:
        pl.semaphore_signal(barrier, inc=1, device_id={"sp": peers[flip]}, device_id_type=MESH)
    own_in = pltpu.make_async_copy(x_ref.at[pl.ds(me * seqs, seqs)], xin.at[:, pl.ds(me * seq_dev, seq_dev)], own_sem.at[0])
    own_in.start()
    for which in range(4):
        weight_copy(0, which).start()
    zeros_z = jnp.zeros((ZPAD, 128), BF16)
    zeros_h = jnp.zeros((HPAD, 128), F32)
    for b in range(seqs):
        for side in range(2):
            u_buf[side, b, 0:ZPAD, :] = zeros_z
            h_buf[side, b, 0:HPAD, :] = zeros_h
        skip[b] = jnp.zeros((seq_len, 128), F32)
    pl.semaphore_wait(barrier, group_n - 1)

    in_copies = [[] for _ in range(GROUPS)]
    for g in range(GROUPS):
        for flip in order:
            peer = peers[flip]
            copy = pltpu.make_async_remote_copy(
                src_ref=x_ref.at[pl.ds(peer * seqs + g * part, part)],
                dst_ref=xin.at[pl.ds(g * part, part), pl.ds(me * seq_dev, seq_dev)],
                send_sem=in_send.at[g, flip - 1], recv_sem=in_recv.at[g, flip - 1], device_id={"sp": peer}, device_id_type=MESH)
            copy.start()
            in_copies[g].append(copy)
    for stack in range(1, stacks):
        for which in range(4):
            weight_copy(stack, which).start()

    own_in.wait()

    def past(side, b, first, rows, dilation):
        if dilation < 16:
            start = HPAD + first - dilation
            return h_buf[side, b, start:start + rows, :].astype(BF16)
        start = ZPAD + first - dilation
        return u_buf[side, b, start:start + rows, :]

    def load_input(g):
        for copy in in_copies[g]:
            copy.wait()
        for b in range(g * part, (g + 1) * part):
            for q in range(seq_len // ROWS):
                piece = xin[b, q * ROWS:(q + 1) * ROWS, :]
                u_buf[0, b, ZPAD + q * ROWS:ZPAD + (q + 1) * ROWS, :] = piece
                h_buf[0, b, HPAD + q * ROWS:HPAD + (q + 1) * ROWS, :] = piece.astype(F32)

    def run(streams, rows, lag1, lag2, paired=True):
        tasks = []
        for k in range(max(len(layers) for _, layers in streams)):
            for g, layers in streams:
                per = max(len(other) for _, other in streams) // len(layers)
                cells = [(b, q) for q in range(seq_len // rows) for b in range(g * part, (g + 1) * part)]
                share = len(cells) // per
                stack, layer = layers[k // per]
                tasks += [(stack, layer, b, q) for b, q in cells[k % per * share:(k % per + 1) * share]]
        zs, rs, gs = {}, {}, []

        def do_z(stack, layer, b, q):
            side = layer % 2
            u = u_buf[side, b, ZPAD + q * rows:ZPAD + (q + 1) * rows, :]
            lhs = jnp.concatenate([u, past(side, b, q * rows, rows, 2 ** layer)], axis=1)
            zs[b, q] = jnp.dot(lhs, jnp.concatenate([wc[stack, layer], wp[stack, layer]], axis=0), preferred_element_type=F32)

        def do_gate(stack, layer, b, q):
            z = zs.pop((b, q))
            a = (jnp.tanh(z[:, :128]) * jax.nn.sigmoid(z[:, 128:])).astype(BF16)
            span = slice(q * rows, (q + 1) * rows)
            w_res = wr[stack, layer]
            zero = jnp.zeros_like(w_res)
            if not paired:
                r = jnp.dot(a, jnp.concatenate([w_res, ws[stack, layer]], axis=1), preferred_element_type=F32)
                rs[b, q] = r[:, :128], r[:, 128:]
            elif layer % 2 == 0:
                a_buf[b, span, :] = a
                gs.append(((b, q), a))
                if len(gs) == 2:
                    (cell0, a0), (cell1, a1) = gs
                    gs.clear()
                    diag = jnp.concatenate([jnp.concatenate([w_res, zero], axis=1), jnp.concatenate([zero, w_res], axis=1)], axis=0)
                    r = jnp.dot(jnp.concatenate([a0, a1], axis=1), diag, preferred_element_type=F32)
                    rs[cell0] = r[:, :128], None
                    rs[cell1] = r[:, 128:], None
            else:
                top = jnp.concatenate([zero, ws[stack, layer - 1]], axis=1)
                rhs = jnp.concatenate([top, jnp.concatenate([w_res, ws[stack, layer]], axis=1)], axis=0)
                r = jnp.dot(jnp.concatenate([a_buf[b, span, :], a], axis=1), rhs, preferred_element_type=F32)
                rs[b, q] = r[:, :128], r[:, 128:]

        def do_update(stack, layer, b, q):
            side = layer % 2
            dh, ds = rs.pop((b, q))
            h_rows = slice(HPAD + q * rows, HPAD + (q + 1) * rows)
            h_new = h_buf[side, b, h_rows, :] + dh
            h_buf[1 - side, b, h_rows, :] = h_new
            u_buf[1 - side, b, ZPAD + q * rows:ZPAD + (q + 1) * rows, :] = h_new.astype(BF16)
            if ds is not None:
                s_rows = slice(q * rows, (q + 1) * rows)
                skip[b, s_rows, :] = skip[b, s_rows, :] + ds

        for k in range(len(tasks) + lag2):
            if k < len(tasks):
                do_z(*tasks[k])
            if 0 <= k - lag1 < len(tasks):
                do_gate(*tasks[k - lag1])
            if 0 <= k - lag2 < len(tasks):
                do_update(*tasks[k - lag2])

    def layers_of(stack):
        return [(stack, layer) for layer in range(cycle_len)]

    def first_use(stack):
        for which in range(4):
            weight_copy(stack, which).wait()

    copies = []

    def send_output(g):
        group_rows = pl.ds(g * part, part)
        pairs = ((h_st, h_out), (s_st, s_out))

        def stage(peer):
            for b in range(g * part, (g + 1) * part):
                h_st[peer, b] = h_buf[0, b, pl.ds(HPAD + peer, seq_dev, stride=group_n), :]
                s_st[peer, b] = skip[b, pl.ds(peer, seq_dev, stride=group_n), :]

        def send(flip):
            for which, (src, dst) in enumerate(pairs):
                copy = pltpu.make_async_remote_copy(
                    src_ref=src.at[peers[flip], group_rows], dst_ref=dst.at[pl.ds(me * seqs + g * part, part)],
                    send_sem=out_send.at[g, which, flip - 1], recv_sem=out_recv.at[g, which, flip - 1],
                    device_id={"sp": peers[flip]}, device_id_type=MESH)
                copy.start()
                copies.append(copy)

        for place, flip in enumerate(order):
            stage(peers[flip])
            if place:
                send(order[place - 1])
        stage(me)
        send(order[-1])
        for which, (src, dst) in enumerate(pairs):
            copy = pltpu.make_async_copy(src.at[me, group_rows], dst.at[pl.ds(me * seqs + g * part, part)], own_sem.at[1 + 2 * g + which])
            copy.start()
            copies.append(copy)

    ahead = LEAD - HEAD
    level = stacks - HEAD - 2 * ahead

    def only_first(stack, carry):
        first_use(stack)
        run([(0, layers_of(stack))], *SOLO)
        return carry

    def two_to_one(k, carry):
        stack = HEAD + 2 * k
        first_use(stack)
        first_use(stack + 1)
        run([(0, layers_of(stack) + layers_of(stack + 1)), (1, layers_of(k))], *FAST)
        return carry

    def one_to_one(k, carry):
        first_use(HEAD + 2 * ahead + k)
        run([(0, layers_of(HEAD + 2 * ahead + k)), (1, layers_of(ahead + k))], *BOTH)
        return carry

    def only_second(stack, carry):
        run([(1, layers_of(stack))], *SOLO)
        return carry

    load_input(0)
    lax.fori_loop(0, HEAD, only_first, 0)
    load_input(1)
    lax.fori_loop(0, ahead, two_to_one, 0)
    lax.fori_loop(0, level, one_to_one, 0)
    send_output(0)
    lax.fori_loop(ahead + level, stacks, only_second, 0)
    send_output(1)
    for copy in copies:
        copy.wait()


def solution(mesh):
    group_n = mesh.shape["sp"]

    def local(x_loc, w_cur, w_past, w_res, w_skip):
        batch, seq_dev, channels = x_loc.shape
        stacks, cycle_len = w_cur.shape[:2]
        seqs, seq_len = batch // group_n, seq_dev * group_n
        any_spec = pl.BlockSpec(memory_space=pl.ANY)
        out = jax.ShapeDtypeStruct((batch, seq_dev, channels), F32)
        args = [pltpu.with_memory_space_constraint(v, pltpu.HBM) for v in (x_loc, w_cur, w_past, w_res, w_skip)]
        h_out, s_out = pl.pallas_call(
            functools.partial(kernel, group_n, seqs, seq_len, stacks, cycle_len),
            out_shape=(out, out),
            in_specs=[any_spec] * 5,
            out_specs=(any_spec, any_spec),
            scratch_shapes=[
                pltpu.VMEM((seqs, seq_len, channels), BF16),
                pltpu.VMEM((2, seqs, HPAD + seq_len, channels), F32),
                pltpu.VMEM((2, seqs, ZPAD + seq_len, channels), BF16),
                pltpu.VMEM((seqs, seq_len, channels), BF16),
                pltpu.VMEM((seqs, seq_len, channels), F32),
                pltpu.VMEM(w_cur.shape, BF16),
                pltpu.VMEM(w_past.shape, BF16),
                pltpu.VMEM(w_res.shape, BF16),
                pltpu.VMEM(w_skip.shape, BF16),
                pltpu.VMEM((group_n, seqs, seq_dev, channels), F32),
                pltpu.VMEM((group_n, seqs, seq_dev, channels), F32),
                pltpu.SemaphoreType.DMA((GROUPS, group_n - 1)),
                pltpu.SemaphoreType.DMA((GROUPS, group_n - 1)),
                pltpu.SemaphoreType.DMA((GROUPS, 2, group_n - 1)),
                pltpu.SemaphoreType.DMA((GROUPS, 2, group_n - 1)),
                pltpu.SemaphoreType.DMA((4, stacks)),
                pltpu.SemaphoreType.DMA((1 + 2 * GROUPS,)),
            ],
            compiler_params=pltpu.CompilerParams(collective_id=0, has_side_effects=True, vmem_limit_bytes=VMEM_MIB * 1024 * 1024),
        )(*args)
        return h_out.reshape(batch, 1, seq_dev, channels), s_out.reshape(batch, 1, seq_dev, channels)

    return jax.shard_map(local, mesh=mesh, in_specs=(P("dp", "sp", None), P(), P(), P(), P()), out_specs=(P("dp", "sp", None, None), P("dp", "sp", None, None)), check_vma=False)
```
